32 devices in a mesh: dp: 4 (over z), row: 2 (over y), col: 4 (over x, core).
Axes of the slice: x: 2, y: 2, z: 4, core: 2. Of those that a mesh axis runs over, the one named last changes fastest.
Arguments:
- block_input: bfloat16 [18816, 512], P(('dp', 'row')), may hold values from -6 to 6
- cotangent: bfloat16 [18816, 512], P(('dp', 'row')), may hold values from -6 to 6
- region_ids: int32 [196], replicated, may hold values from 0 to 3
- rel_index: int32 [49, 49], replicated, may hold values from 0 to 168
- first_gain: float32 [2, 512], replicated, may hold values from 0.5 to 1.5
- first_offset: float32 [2, 512], replicated, may hold values from -3 to 3
- triple_weight: bfloat16 [2, 512, 3, 512], P(None, 'row', None, 'col'), may hold values from -0.25 to 0.25
- triple_bias: float32 [2, 3, 512], P(None, None, 'col'), may hold values from -3 to 3
- rel_table: float32 [2, 169, 16], P(None, None, 'col'), may hold values from -4 to 4
- project_weight: bfloat16 [2, 512, 512], P(None, 'row', 'col'), may hold values from -0.375 to 0.375
- project_bias: float32 [2, 512], replicated, may hold values from -3 to 3
- second_gain: float32 [2, 512], replicated, may hold values from 0.5 to 1.5
- second_offset: float32 [2, 512], replicated, may hold values from -3 to 3
- expand_weight: bfloat16 [2, 512, 2048], P(None, 'row', 'col'), may hold values from -0.25 to 0.25
- expand_bias: float32 [2, 2048], P(None, 'col'), may hold values from -3 to 3
- reduce_weight: bfloat16 [2, 512, 2048], P(None, 'row', 'col'), may hold values from -0.125 to 0.125
- reduce_bias: float32 [2, 512], replicated, may hold values from -3 to 3
Outputs:
- block_output: float32 [18816, 512], P(('dp', 'row'))
- input_grad: float32 [18816, 512], P(('dp', 'row'))
- first_gain_grad: float32 [2, 512], replicated
- first_offset_grad: float32 [2, 512], replicated
- triple_weight_grad: float32 [2, 512, 3, 512], P(None, 'row', None, 'col')
- triple_bias_grad: float32 [2, 3, 512], P(None, None, 'col')
- rel_table_grad: float32 [2, 169, 16], P(None, None, 'col')
- project_weight_grad: float32 [2, 512, 512], P(None, 'row', 'col')
- project_bias_grad: float32 [2, 512], replicated
- second_gain_grad: float32 [2, 512], replicated
- second_offset_grad: float32 [2, 512], replicated
- expand_weight_grad: float32 [2, 512, 2048], P(None, 'row', 'col')
- expand_bias_grad: float32 [2, 2048], P(None, 'col')
- reduce_weight_grad: float32 [2, 512, 2048], P(None, 'row', 'col')
- reduce_bias_grad: float32 [2, 512], replicated
The draws below stay inside these ranges and needn't reach their ends.
Inputs may be any that keep to these rules, and one draw needn't show every extreme that they name: region_ids[p] is the region of position p of the rolled 14 x 14 grid, row-major. rel_index[i, j] selects the row of rel_table for query position i and key position j of a window, both row-major.
All inputs are finite; a program needn't handle non-finite values.
Results may differ from the reference program's by a relative error of at most 0.038.
Values may be sent and summed in bfloat16 or wider, within the bound.
A program may use at most 192 MiB of HBM per device.

```python
import math
import jax
import jax.numpy as jnp
from jax import lax

D = 512
HEADS = 16
FF = 2048
LAYERS = 2
SIDE = 14
WIN = 7
SHIFT = 3
HEAD = 32
RELS = 169
PIECES = 4
TOK_DEV = 2352
TOKENS = 18816
N_DP = 4
N_ROW = 2


def place_ends(values, rng, least, largest):
    index_at = [jax.random.randint(jax.random.fold_in(rng, axis), (), 0, length) for axis, length in enumerate(values.shape)]
    widest = values.shape.index(max(values.shape))
    beside = index_at[:widest] + [(index_at[widest] + 1) % values.shape[widest]] + index_at[widest + 1:]
    return values.at[tuple(index_at)].set(least).at[tuple(beside)].set(largest)


def level_of(own_key, shape, pieces, low, top_value):
    level, own = 1.0, jax.random.fold_in(own_key, 6)
    for axis_at, shards_of in pieces:
        draws = jnp.exp(jax.random.uniform(jax.random.fold_in(own, axis_at), (shards_of,), jnp.float32, low / len(pieces), top_value / len(pieces)))
        level = level * jnp.repeat(draws, shape[axis_at] // shards_of).reshape([-1 if axis == axis_at else 1 for axis in range(len(shape))])
    return level


def centred(stream_key, shape, spread, bound, cuts=(), held_as=jnp.bfloat16):
    factor_of = level_of(stream_key, shape, cuts, -0.22, 0.18) if cuts else 1.0
    entries = jax.random.normal(stream_key, shape, jnp.float32) * spread * factor_of
    return jnp.minimum(jnp.maximum(entries, -bound), bound).astype(held_as)


def setup_inputs(seed: int = 0) -> dict:
    keys = jax.random.split(jax.random.key(seed), 18)
    block_input = centred(keys[0], (TOKENS, D), 1.0, 6.0, ((0, 8),))
    cotangent = centred(keys[1], (TOKENS, D), 1.0, 6.0, ((0, 8),))
    region_ids = place_ends(jax.random.randint(keys[2], (SIDE * SIDE,), 0, 4), jax.random.fold_in(keys[2], 1), 0, 3).astype(jnp.int32)
    rel_index = place_ends(jax.random.randint(keys[3], (WIN * WIN, WIN * WIN), 0, RELS), jax.random.fold_in(keys[3], 1), 0, RELS - 1).astype(jnp.int32)
    first_gain = jnp.clip(1.0 + 0.1 * jax.random.normal(keys[4], (LAYERS, D), jnp.float32), 0.5, 1.5)
    first_offset = centred(keys[5], (LAYERS, D), 0.5, 3.0, (), jnp.float32)
    triple_weight = centred(keys[6], (LAYERS, D, 3, D), D ** -0.5, 0.25, ((1, 2), (3, 4)))
    triple_bias = centred(keys[7], (LAYERS, 3, D), 0.5, 3.0, ((2, 4),), jnp.float32)
    rel_table = centred(keys[8], (LAYERS, RELS, HEADS), 1.0, 4.0, ((2, 4),), jnp.float32)
    project_weight = centred(keys[9], (LAYERS, D, D), (D // 2) ** -0.5, 0.375, ((1, 2), (2, 4)))
    project_bias = centred(keys[10], (LAYERS, D), 0.5, 3.0, (), jnp.float32)
    second_gain = jnp.clip(1.0 + 0.1 * jax.random.normal(keys[11], (LAYERS, D), jnp.float32), 0.5, 1.5)
    second_offset = centred(keys[12], (LAYERS, D), 0.5, 3.0, (), jnp.float32)
    expand_weight = centred(keys[13], (LAYERS, D, FF), D ** -0.5, 0.25, ((1, 2), (2, 4)))
    expand_bias = centred(keys[14], (LAYERS, FF), 0.5, 3.0, ((1, 4),), jnp.float32)
    reduce_weight = centred(keys[15], (LAYERS, D, FF), FF ** -0.5, 0.125, ((1, 2), (2, 4)))
    reduce_bias = centred(keys[16], (LAYERS, D), 0.5, 3.0, (), jnp.float32)
    return {"block_input": block_input, "cotangent": cotangent, "region_ids": region_ids, "rel_index": rel_index, "first_gain": first_gain, "first_offset": first_offset, "triple_weight": triple_weight, "triple_bias": triple_bias, "rel_table": rel_table, "project_weight": project_weight, "project_bias": project_bias, "second_gain": second_gain, "second_offset": second_offset, "expand_weight": expand_weight, "expand_bias": expand_bias, "reduce_weight": reduce_weight, "reduce_bias": reduce_bias}


EPSILON = 1e-05
MASKED = -100.0
HIGHEST = lax.Precision.HIGHEST

def layer_norm(hidden, scales, offsets):
    average = lax.optimization_barrier(jnp.mean(hidden, axis=-1, keepdims=True))
    centered = hidden - average
    variance = lax.optimization_barrier(jnp.mean(centered * centered, axis=-1, keepdims=True))
    inverse = lax.rsqrt(variance + EPSILON)
    normed = centered * inverse
    return (normed * scales + offsets, normed, inverse)

def norm_backward(upstream, normed, inverse, scales):
    weighted = upstream * scales
    first_mean = lax.optimization_barrier(jnp.mean(weighted, axis=-1, keepdims=True))
    second_mean = lax.optimization_barrier(jnp.mean(weighted * normed, axis=-1, keepdims=True))
    result = inverse * (weighted - first_mean - normed * second_mean)
    return (result, lax.optimization_barrier(jnp.sum(upstream * normed, axis=0)), lax.optimization_barrier(jnp.sum(upstream, axis=0)))

def gelu_exact(values):
    return jax.nn.gelu(values, approximate=False)

def to_windows(tokens, images, offset):
    blocks = SIDE // WIN
    columns = tokens.shape[-1]
    spatial = tokens.reshape(images, SIDE, SIDE, columns)
    if offset:
        spatial = jnp.roll(spatial, (-offset, -offset), axis=(1, 2))
    spatial = spatial.reshape(images, blocks, WIN, blocks, WIN, columns).transpose(0, 1, 3, 2, 4, 5)
    return spatial.reshape(images * blocks * blocks, WIN * WIN, columns)

def from_windows(windows, images, offset):
    blocks = SIDE // WIN
    columns = windows.shape[-1]
    spatial = windows.reshape(images, blocks, blocks, WIN, WIN, columns).transpose(0, 1, 3, 2, 4, 5)
    spatial = spatial.reshape(images, SIDE, SIDE, columns)
    if offset:
        spatial = jnp.roll(spatial, (offset, offset), axis=(1, 2))
    return spatial.reshape(images * SIDE * SIDE, columns)

def region_mask(region_ids):
    cells = to_windows(region_ids.reshape(SIDE * SIDE, 1), 1, 0)[:, :, 0]
    return jnp.where(cells[:, :, None] == cells[:, None, :], 0.0, MASKED).astype(jnp.float32)

def rel_onehot(rel_index):
    return (rel_index.reshape(-1)[:, None] == jnp.arange(RELS, dtype=jnp.int32)[None, :]).astype(jnp.float32)

def rel_bias(onehot, table):
    count = table.shape[1]
    return jnp.dot(onehot, table, precision=HIGHEST).T.reshape(count, WIN * WIN, WIN * WIN)

def piece_sum(parts):
    rounded = lax.optimization_barrier(parts.astype(jnp.bfloat16))
    return lax.optimization_barrier(jnp.sum(rounded.astype(jnp.float32), axis=0))

def window_scores(query_win, key_win, bias, layer_mask, images):
    scores = jnp.einsum('wihd,wjhd->whij', query_win.astype(jnp.float32), key_win.astype(jnp.float32))
    scores = scores + bias[None]
    if layer_mask is not None:
        shaped = scores.reshape((images, layer_mask.shape[0]) + scores.shape[1:])
        scores = (shaped + layer_mask[None, :, None]).reshape(scores.shape)
    return scores

def attend_forward(query_win, key_win, value_win, bias, layer_mask, images):
    scores = window_scores(query_win, key_win, bias, layer_mask, images)
    log_total = jnp.log(lax.optimization_barrier(jnp.sum(jnp.exp(scores), axis=-1)))
    probs = jnp.exp(scores - log_total[..., None]).astype(jnp.bfloat16)
    output = jnp.einsum('whij,wjhd->wihd', probs.astype(jnp.float32), value_win.astype(jnp.float32))
    return (output.astype(jnp.bfloat16), log_total)

def attend_backward(query_win, key_win, value_win, output, log_total, out_grad, bias, layer_mask, images):
    scores = window_scores(query_win, key_win, bias, layer_mask, images)
    probs = jnp.exp(scores - log_total[..., None])
    probs_low = probs.astype(jnp.bfloat16).astype(jnp.float32)
    grad_wide = out_grad.astype(jnp.float32)
    value_grad = jnp.einsum('whij,wihd->wjhd', probs_low, grad_wide)
    prob_grad = jnp.einsum('wihd,wjhd->whij', grad_wide, value_win.astype(jnp.float32))
    delta = lax.optimization_barrier(jnp.sum(grad_wide * output.astype(jnp.float32), axis=-1)).transpose(0, 2, 1)
    score_grad = probs * (prob_grad - delta[..., None])
    bias_grad = lax.optimization_barrier(jnp.sum(score_grad, axis=0))
    score_low = score_grad.astype(jnp.bfloat16).astype(jnp.float32)
    query_grad = jnp.einsum('whij,wjhd->wihd', score_low, key_win.astype(jnp.float32)) * HEAD ** (-0.5)
    key_grad = jnp.einsum('whij,wihd->wjhd', score_low, query_win.astype(jnp.float32))
    return (query_grad, key_grad, value_grad, bias_grad)

def group_pass(rows, cot_rows, params, onehot, shift_mask):
    first_gain, first_offset, triple_weight, triple_bias, rel_table, project_weight, project_bias, second_gain, second_offset, expand_weight, expand_bias, reduce_weight, reduce_bias = params
    tokens = rows.shape[0]
    images = tokens // (SIDE * SIDE)
    windows = images * (SIDE // WIN) ** 2
    part_width = D // PIECES
    hidden_part = FF // PIECES
    scaling = jnp.array([HEAD ** (-0.5), 1.0, 1.0], dtype=jnp.float32)[:, None]
    hidden = rows.astype(jnp.float32)
    stored = []
    for layer_index in range(LAYERS):
        offset = SHIFT if layer_index % 2 == 1 else 0
        layer_mask = shift_mask if offset else None
        bias = rel_bias(onehot, rel_table[layer_index])
        normed, first_hat, first_inv = layer_norm(hidden, first_gain[layer_index], first_offset[layer_index])
        first_low = normed.astype(jnp.bfloat16)
        triple = jnp.einsum('td,dkc->tkc', first_low.astype(jnp.float32), triple_weight[layer_index].astype(jnp.float32))
        triple_low = ((triple + triple_bias[layer_index]) * scaling).astype(jnp.bfloat16)
        windowed = to_windows(triple_low.reshape(tokens, 3 * D), images, offset)
        windowed = windowed.reshape(windows, WIN * WIN, 3, HEADS, HEAD)
        query_win = windowed[:, :, 0]
        key_win = windowed[:, :, 1]
        value_win = windowed[:, :, 2]
        attn_out, log_total = attend_forward(query_win, key_win, value_win, bias, layer_mask, images)
        merged = from_windows(attn_out.reshape(windows, WIN * WIN, D), images, offset)
        parts = jnp.einsum('tpc,epc->pte', merged.reshape(tokens, PIECES, part_width).astype(jnp.float32), project_weight[layer_index].reshape(D, PIECES, part_width).astype(jnp.float32))
        middle = hidden + piece_sum(parts) + project_bias[layer_index]
        normed, second_hat, second_inv = layer_norm(middle, second_gain[layer_index], second_offset[layer_index])
        second_low = normed.astype(jnp.bfloat16)
        pre_act = jnp.dot(second_low, expand_weight[layer_index], preferred_element_type=jnp.float32) + expand_bias[layer_index]
        act_low = gelu_exact(pre_act).astype(jnp.bfloat16)
        parts = jnp.einsum('tpc,epc->pte', act_low.reshape(tokens, PIECES, hidden_part).astype(jnp.float32), reduce_weight[layer_index].reshape(D, PIECES, hidden_part).astype(jnp.float32))
        stored.append((first_hat, first_inv, first_low, query_win, key_win, value_win, attn_out, log_total, merged, second_hat, second_inv, second_low, pre_act, act_low, bias, layer_mask, offset))
        hidden = middle + piece_sum(parts) + reduce_bias[layer_index]
    grad = cot_rows.astype(jnp.float32)
    collected = [None] * LAYERS
    for layer_index in reversed(range(LAYERS)):
        first_hat, first_inv, first_low, query_win, key_win, value_win, attn_out, log_total, merged, second_hat, second_inv, second_low, pre_act, act_low, bias, layer_mask, offset = stored[layer_index]
        reduce_bias_grad = lax.optimization_barrier(jnp.sum(grad, axis=0))
        grad_low = grad.astype(jnp.bfloat16)
        reduce_weight_grad = jnp.dot(grad_low.T, act_low, preferred_element_type=jnp.float32)
        act_grad = jnp.dot(grad_low, reduce_weight[layer_index], preferred_element_type=jnp.float32)
        pre_grad = jax.vjp(gelu_exact, pre_act)[1](act_grad)[0]
        expand_bias_grad = lax.optimization_barrier(jnp.sum(pre_grad, axis=0))
        pre_low = pre_grad.astype(jnp.bfloat16)
        expand_weight_grad = jnp.dot(second_low.T, pre_low, preferred_element_type=jnp.float32)
        parts = jnp.einsum('tpc,dpc->ptd', pre_low.reshape(tokens, PIECES, hidden_part).astype(jnp.float32), expand_weight[layer_index].reshape(D, PIECES, hidden_part).astype(jnp.float32))
        back, second_gain_grad, second_offset_grad = norm_backward(piece_sum(parts), second_hat, second_inv, second_gain[layer_index])
        grad = grad + back
        project_bias_grad = lax.optimization_barrier(jnp.sum(grad, axis=0))
        grad_low = grad.astype(jnp.bfloat16)
        project_weight_grad = jnp.dot(grad_low.T, merged, preferred_element_type=jnp.float32)
        merged_grad = jnp.dot(grad_low, project_weight[layer_index], preferred_element_type=jnp.float32).astype(jnp.bfloat16)
        out_grad_win = to_windows(merged_grad, images, offset).reshape(windows, WIN * WIN, HEADS, HEAD)
        query_grad, key_grad, value_grad, bias_grad = attend_backward(query_win, key_win, value_win, attn_out, log_total, out_grad_win, bias, layer_mask, images)
        rel_table_grad = jnp.dot(onehot.T, bias_grad.reshape(HEADS, -1).T, precision=HIGHEST)
        stacked = jnp.stack((query_grad, key_grad, value_grad), axis=2).reshape(windows, WIN * WIN, 3 * D)
        triple_grad = from_windows(stacked, images, offset).reshape(tokens, 3, D)
        triple_bias_grad = lax.optimization_barrier(jnp.sum(triple_grad, axis=0))
        triple_low_grad = triple_grad.astype(jnp.bfloat16)
        triple_weight_grad = jnp.einsum('td,tkc->dkc', first_low.astype(jnp.float32), triple_low_grad.astype(jnp.float32))
        parts = jnp.einsum('tkpc,dkpc->ptd', triple_low_grad.reshape(tokens, 3, PIECES, part_width).astype(jnp.float32), triple_weight[layer_index].reshape(D, 3, PIECES, part_width).astype(jnp.float32))
        back, first_gain_grad, first_offset_grad = norm_backward(piece_sum(parts), first_hat, first_inv, first_gain[layer_index])
        grad = grad + back
        collected[layer_index] = (first_gain_grad, first_offset_grad, triple_weight_grad, triple_bias_grad, rel_table_grad, project_weight_grad, project_bias_grad, second_gain_grad, second_offset_grad, expand_weight_grad, expand_bias_grad, reduce_weight_grad, reduce_bias_grad)
    grads = tuple((jnp.stack([collected[index][slot] for index in range(LAYERS)]) for slot in range(13)))
    return (hidden, grad, grads)

def reference(block_input, cotangent, region_ids, rel_index, first_gain, first_offset, triple_weight, triple_bias, rel_table, project_weight, project_bias, second_gain, second_offset, expand_weight, expand_bias, reduce_weight, reduce_bias):
    params = (first_gain, first_offset, triple_weight, triple_bias, rel_table, project_weight, project_bias, second_gain, second_offset, expand_weight, expand_bias, reduce_weight, reduce_bias)
    onehot = rel_onehot(rel_index)
    shift_mask = region_mask(region_ids)
    groups = N_DP * N_ROW
    rows_in = block_input.reshape(groups, TOK_DEV, D)
    cot_in = cotangent.reshape(groups, TOK_DEV, D)
    zeros = tuple((jnp.zeros(param.shape, jnp.float32) for param in params))

    def advance(carry, inputs):
        output, in_grad, grads = group_pass(inputs[0], inputs[1], params, onehot, shift_mask)
        return (jax.tree.map(jnp.add, carry, grads), (output, in_grad))
    totals, outputs = lax.scan(advance, zeros, (rows_in, cot_in))
    grad_scale = 1.0 / math.sqrt(TOKENS)
    totals = tuple((total * grad_scale for total in totals))
    block_output = outputs[0].reshape(TOKENS, D)
    input_grad = outputs[1].reshape(TOKENS, D)
    return (block_output, input_grad, totals[0], totals[1], totals[2], totals[3], totals[4], totals[5], totals[6], totals[7], totals[8], totals[9], totals[10], totals[11], totals[12])
```

```python
import functools
import math

import jax
import jax.numpy as jnp
from jax import lax
from jax.experimental import pallas as pl
from jax.experimental.pallas import tpu as pltpu
from jax.sharding import PartitionSpec as P

LAYERS = 2
SIDE = 14
WIN = 7
SHIFT = 3
HEAD = 32
RELS = 169
EPSILON = 1e-05
MASKED = -100.0
GONE = -1e30
CELLS = WIN * WIN
ROWS = 56
SLOT = 64
GROUP = 4
LANES = 128
WIDE = GROUP * SLOT
F32 = jnp.float32
BF16 = jnp.bfloat16
ROOT_HALF = 1.0 / math.sqrt(2.0)
GAUSS = 1.0 / math.sqrt(2.0 * math.pi)


def mm(a, b):
    return lax.dot_general(a, b, (((1,), (0,)), ((), ())), preferred_element_type=F32)


def mm_nt(a, b):
    return lax.dot_general(a, b, (((1,), (1,)), ((), ())), preferred_element_type=F32)


def mm_tn(a, b):
    return lax.dot_general(a, b, (((0,), (0,)), ((), ())), preferred_element_type=F32)


def loop(count, body):
    def step(index, carry):
        body(index)
        return carry

    lax.fori_loop(0, count, step, 0)


def span(index, size):
    return pl.ds(pl.multiple_of(index * size, size), size)


def fold(values):
    rows, columns = values.shape
    return jnp.sum(values.reshape(rows // 8, 8, columns), axis=0)


def order(images, shift):
    found = {}
    for image in range(images):
        for wi in range(2):
            for wj in range(2):
                window = image * 4 + wi * 2 + wj
                for a in range(WIN):
                    for b in range(WIN):
                        i = (wi * WIN + a + shift) % SIDE
                        j = (wj * WIN + b + shift) % SIDE
                        found[window * ROWS + a * WIN + b] = image * SIDE * SIDE + i * SIDE + j
    return found


def runs(pairs):
    joined = []
    for to, source in sorted(pairs):
        if joined and joined[-1][0] + joined[-1][2] == to and joined[-1][1] + joined[-1][2] == source:
            joined[-1][2] += 1
        else:
            joined.append([to, source, 1])
    return joined


def image_to_window(images, shift):
    return runs(order(images, shift).items())


def window_to_image(images, shift):
    return runs((source, to) for to, source in order(images, shift).items())


def window_to_window(images, before, after):
    at = {token: row for row, token in order(images, before).items()}
    return runs((row, at[token]) for row, token in order(images, after).items())


def move_rows(target, source, moves):
    for to, start, length in moves:
        target[pl.ds(to, length), :] = source[pl.ds(start, length), :]


def norm_rows(hidden, gain, offset):
    average = jnp.mean(hidden, axis=-1, keepdims=True)
    centered = hidden - average
    variance = jnp.mean(centered * centered, axis=-1, keepdims=True)
    inverse = lax.rsqrt(variance + EPSILON)
    normed = centered * inverse
    return normed * gain + offset, normed, inverse


def spread(block, mask):
    return jnp.concatenate([block] * GROUP, axis=0) * mask


def gather_heads(stacked, lane):
    out = stacked[(GROUP - 1) * SLOT :]
    for head in reversed(range(GROUP - 1)):
        out = jnp.where(lane < (head + 1) * HEAD, stacked[head * SLOT : (head + 1) * SLOT], out)
    return out


def padded(rows):
    return jnp.concatenate([rows, jnp.zeros((SLOT - ROWS, rows.shape[1]), rows.dtype)], axis=0).astype(BF16)


class Sizes:
    def __init__(self, images, width, hidden):
        self.images = images
        self.windows = images * 4
        self.tokens = self.windows * ROWS
        self.width = width
        self.hidden = hidden
        self.groups = width // LANES
        self.pairs = self.windows // 2
        self.chunk = self.tokens // 2
        self.third = self.tokens // 3


def forward_norm(sz, hidden, gain, offset, low, hat, inv):
    def body(i):
        at = span(i, 2 * ROWS)
        normed, centered, inverse = norm_rows(hidden[at, :], gain, offset)
        low[at, :] = normed.astype(BF16)
        hat[at, :] = centered.astype(BF16)
        inv[at, :] = inverse

    loop(sz.pairs, body)


def forward_triple(sz, low, weight, bias, outs):
    per = sz.chunk // ROWS
    for part in range(3):

        def body(i, part=part):
            acc = mm(low[span(i, sz.chunk), :], weight[part]) + bias[part : part + 1, :]
            if part == 0:
                acc = acc * HEAD ** (-0.5)
            for j in range(per):
                outs[part][i * per + j] = padded(acc[j * ROWS : (j + 1) * ROWS])

        loop(2, body)


def forward_attend(sz, parts, bias, mask, heads, ones, probs, out_slots, out_rows):
    query, key, value = parts

    def body(pair):
        for group in range(sz.groups):
            cols = slice(group * LANES, (group + 1) * LANES)
            halves = []
            for half in range(2):
                window = pair * 2 + half
                scores = mm_nt(query[window, :, cols], spread(key[window, :, cols], heads[...])) + bias[group]
                if mask is not None:
                    scores = scores + mask[lax.rem(window, 4)]
                grown = jnp.exp(scores)
                high = grown.astype(BF16)
                low = (grown - high.astype(F32)).astype(BF16)
                total = mm(high, ones[...]) + mm(low, ones[...])
                prob = jnp.exp(scores - jnp.log(total)).astype(BF16)
                probs[window, group] = prob
                out = mm(prob, spread(value[window, :, cols], heads[...]))
                out_slots[window, :, cols] = out.astype(BF16)
                halves.append(out[:ROWS])
            out_rows[span(pair, 2 * ROWS), cols] = jnp.concatenate(halves, axis=0).astype(BF16)

    loop(sz.pairs, body)


def add_product(sz, hidden, left, weight, bias):
    def body(i):
        at = span(i, sz.chunk)
        hidden[at, :] = hidden[at, :] + mm_nt(left[at, :], weight[...]) + bias

    loop(2, body)


def forward_expand(sz, low, weight, bias, act, slope):
    parts = sz.hidden // sz.width

    def body(i):
        rows = span(i // parts, sz.third)
        cols = span(lax.rem(i, parts), sz.width)
        u = mm(low[rows, :], weight[:, cols]) + bias[:, cols]
        phi = 0.5 + 0.5 * lax.erf(u * ROOT_HALF)
        act[rows, cols] = (u * phi).astype(BF16)
        slope[rows, cols] = (phi + u * (GAUSS * jnp.exp(-0.5 * u * u))).astype(BF16)

    loop(3 * parts, body)


def backward_norm(sz, upstream, grad, hat, inv, gain, sums):
    def body(i):
        at = span(i, 2 * ROWS)
        up = upstream[at, :]
        normed = hat[at, :].astype(F32)
        weighted = up * gain
        first = jnp.mean(weighted, axis=-1, keepdims=True)
        second = jnp.mean(weighted * normed, axis=-1, keepdims=True)
        grad[at, :] = grad[at, :] + inv[at, :] * (weighted - first - normed * second)
        sums[0] += fold(up * normed)
        sums[1] += fold(up)

    sums[0] = jnp.zeros_like(sums[0])
    sums[1] = jnp.zeros_like(sums[1])
    loop(sz.pairs, body)


def round_grad(sz, grad, low, low_t, total):
    total[...] = jnp.zeros_like(total)

    def body(i):
        at = span(i, 2 * ROWS)
        values = grad[at, :]
        low[at, :] = values.astype(BF16)
        total[...] += fold(values)

    loop(sz.pairs, body)


def backward_hidden(sz, grad_low, weight, slope, pre_low, total):
    parts = sz.hidden // sz.width
    total[...] = jnp.zeros_like(total)

    def body(i):
        rows = span(i // parts, sz.third)
        cols = span(lax.rem(i, parts), sz.width)
        pre = mm(grad_low[rows, :], weight[:, cols]) * slope[rows, cols].astype(F32)
        pre_low[rows, cols] = pre.astype(BF16)
        total[:, cols] += fold(pre)

    loop(3 * parts, body)


def weight_grad(parts, left, right, width, out, scale):
    def body(i):
        cols = span(i, width)
        out[:, cols] = (mm_tn(left[...], right[:, cols]) * scale).astype(out.dtype)

    loop(parts, body)


def backward_out(sz, grad_low, weight, out_slots):
    per = sz.chunk // ROWS

    def body(i):
        acc = mm(grad_low[span(i, sz.chunk), :], weight[...])
        for j in range(per):
            out_slots[i * per + j] = padded(acc[j * ROWS : (j + 1) * ROWS])

    loop(2, body)


def backward_attend(sz, parts, probs, out_slots, grad_slots, heads, lane, outs, totals, score_sum):
    query, key, value = parts
    for group in range(sz.groups):
        score_sum[group] = jnp.zeros_like(score_sum[group])
    totals[...] = jnp.zeros_like(totals)

    def body(pair):
        for group in range(sz.groups):
            cols = slice(group * LANES, (group + 1) * LANES)
            halves = [[], [], []]
            for half in range(2):
                window = pair * 2 + half
                q, k, v = query[window, :, cols], key[window, :, cols], value[window, :, cols]
                prob = probs[window, group]
                grad = grad_slots[window, :, cols]
                inner = -(grad.astype(F32) * out_slots[window, :, cols].astype(F32))
                left = jnp.concatenate([grad, inner.astype(BF16)], axis=1)
                right = jnp.concatenate([spread(v, heads[...]), heads[...]], axis=1)
                score = prob.astype(F32) * mm_nt(left, right)
                score_sum[group] += score
                score_low = score.astype(BF16)
                halves[0].append((mm(score_low, spread(k, heads[...])) * HEAD ** (-0.5))[:ROWS])
                halves[1].append(gather_heads(mm_tn(score_low, q), lane)[:ROWS])
                halves[2].append(gather_heads(mm_tn(prob, grad), lane)[:ROWS])
            for part in range(3):
                joined = jnp.concatenate(halves[part], axis=0)
                outs[part, span(pair, 2 * ROWS), cols] = joined.astype(BF16)
                totals[part, :, cols] += fold(joined)

    loop(sz.pairs, body)


def back_product(sz, lefts, weights, out):
    def body(i):
        at = span(i, sz.chunk)
        total = mm_nt(lefts[0][at, :], weights[0][...])
        for left, weight in zip(lefts[1:], weights[1:]):
            total = total + mm_nt(left[at, :], weight[...])
        out[at, :] = total

    loop(2, body)


def to_windows(tokens, images, offset):
    blocks = SIDE // WIN
    columns = tokens.shape[-1]
    spatial = tokens.reshape(images, SIDE, SIDE, columns)
    if offset:
        spatial = jnp.roll(spatial, (-offset, -offset), axis=(1, 2))
    spatial = spatial.reshape(images, blocks, WIN, blocks, WIN, columns).transpose(0, 1, 3, 2, 4, 5)
    return spatial.reshape(images * blocks * blocks, WIN * WIN, columns)


def region_mask(region_ids):
    cells = to_windows(region_ids.reshape(SIDE * SIDE, 1), 1, 0)[:, :, 0]
    return jnp.where(cells[:, :, None] == cells[:, None, :], 0.0, MASKED).astype(jnp.float32)


def rel_onehot(rel_index):
    return (rel_index.reshape(-1)[:, None] == jnp.arange(RELS, dtype=jnp.int32)[None, :]).astype(jnp.float32)


def rel_bias(onehot, table):
    count = table.shape[1]
    return jnp.dot(onehot, table, precision=lax.Precision.HIGHEST).T.reshape(count, WIN * WIN, WIN * WIN)


def head_mask():
    row = lax.broadcasted_iota(jnp.int32, (WIDE, LANES), 0) // SLOT
    col = lax.broadcasted_iota(jnp.int32, (WIDE, LANES), 1) // HEAD
    return jnp.where(row == col, 1.0, 0.0).astype(BF16)

def ones_mask():
    row = lax.broadcasted_iota(jnp.int32, (WIDE, WIDE), 0) // SLOT
    col = lax.broadcasted_iota(jnp.int32, (WIDE, WIDE), 1) // SLOT
    return jnp.where(row == col, 1.0, 0.0).astype(BF16)

def forward_kernel(sz, x, wt, wp, we, wr, fg, fo, tb, pb, sg, so, eb, rb, bias, mask, heads, ones,
                   out, n1, xh1, r1, q, k, v, probs, o64, oc, n2, xh2, r2, gp, act, ha, hb):
    move = [image_to_window(sz.images, 0), window_to_window(sz.images, 0, SHIFT), window_to_image(sz.images, SHIFT)]
    hb[...] = jnp.zeros_like(hb)
    ha[...] = jnp.zeros_like(ha)
    hb[0:592, :] = x[...].astype(F32)
    move_rows(ha, hb, move[0])
    bufs = [ha, hb]
    for l in range(2):
        h = bufs[l]
        forward_norm(sz, h, fg[l:l+1, :], fo[l:l+1, :], n1.at[l], xh1.at[l], r1.at[l])
        forward_triple(sz, n1.at[l], wt.at[l], tb.at[l], (q.at[l], k.at[l], v.at[l]))
        forward_attend(sz, (q.at[l], k.at[l], v.at[l]), bias.at[l], mask if l else None, heads, ones, probs.at[l], o64.at[l], oc.at[l])
        add_product(sz, h, oc.at[l], wp.at[l], pb[l:l+1, :])
        forward_norm(sz, h, sg[l:l+1, :], so[l:l+1, :], n2.at[l], xh2.at[l], r2.at[l])
        forward_expand(sz, n2.at[l], we.at[l], eb.at[l:l+1], act.at[l], gp.at[l])
        add_product(sz, h, act.at[l], wr.at[l], rb[l:l+1, :])
        if l == 0:
            hb[...] = jnp.zeros_like(hb)
            move_rows(hb, ha, move[1])
        else:
            move_rows(ha, hb, move[2])
            out[...] = ha[0:592, :]

def backward_kernel(sz, scale, which, cot, wt, wp, we, wr, fg, sg, heads, n1, xh1, r1, q, k, v, probs, o64, oc, n2, xh2, r2, gp, act,
                    out, gt, gp_, ge, gr, small, big, tsum, ssum, ga, gb, low, pre, dn, do64, dc, sums):
    move = [image_to_window(sz.images, SHIFT), window_to_window(sz.images, SHIFT, 0), window_to_image(sz.images, 0)]
    ga[...] = jnp.zeros_like(ga); gb[...] = jnp.zeros_like(gb)
    if which:
        ga[0:592, :] = cot[...].astype(F32)
        move_rows(gb, ga, move[0])
    else:
        gb[...] = cot[...]
    lane = lax.broadcasted_iota(jnp.int32, (SLOT, LANES), 1)
    l = 0
    e = gb
    round_grad(sz, e, low, None, small.at[l, 0])
    weight_grad(4, low, act.at[l], sz.width, gr.at[l], scale)
    backward_hidden(sz, low, wr.at[l], gp.at[l], pre, big.at[l])
    weight_grad(4, n2.at[l], pre, sz.width, ge.at[l], scale)
    back_product(sz, [pre], [we.at[l]], dn)
    backward_norm(sz, dn, e, xh2.at[l], r2.at[l], sg[l:l+1, :], small.at[l, 1:3])
    round_grad(sz, e, low, None, small.at[l, 3])
    weight_grad(1, low, oc.at[l], sz.width, gp_.at[l], scale)
    backward_out(sz, low, wp.at[l], do64)
    backward_attend(sz, (q.at[l], k.at[l], v.at[l]), probs.at[l], o64.at[l], do64, heads, lane, dc, tsum.at[l], ssum.at[l])
    for part in range(3):
        weight_grad(1, n1.at[l], dc.at[part], sz.width, gt.at[l, part], scale)
    back_product(sz, [dc.at[p] for p in range(3)], [wt.at[l, p] for p in range(3)], dn)
    backward_norm(sz, dn, e, xh1.at[l], r1.at[l], fg[l:l+1, :], small.at[l, 4:6])
    ga[...] = jnp.zeros_like(ga)
    if which:
        move_rows(ga, gb, move[1])
        out[...] = ga[...]
    else:
        move_rows(ga, gb, move[2])
        out[...] = ga[...]

LIMIT = 66_900_000
def saved_shapes(sz):
    L, T, D, W = 2, sz.tokens, sz.width, sz.windows
    return [((L,T,D),BF16),((L,T,D),BF16),((L,T,1),F32),((L,W,SLOT,D),BF16),((L,W,SLOT,D),BF16),((L,W,SLOT,D),BF16),
            ((L,W,sz.groups,SLOT,WIDE),BF16),((L,W,SLOT,D),BF16),((L,T,D),BF16),((L,T,D),BF16),((L,T,D),BF16),((L,T,1),F32),
            ((L,T,sz.hidden),BF16),((L,T,sz.hidden),BF16)]
VM = pl.BlockSpec(memory_space=pltpu.VMEM)

def fwd_call(sz, *args):
    shapes = [((592, sz.width), F32)] + saved_shapes(sz)
    return pl.pallas_call(functools.partial(forward_kernel, sz),
        out_shape=[jax.ShapeDtypeStruct(s, d) for s, d in shapes],
        in_specs=[VM]*len(args), out_specs=[VM]*len(shapes),
        scratch_shapes=[pltpu.VMEM((sz.tokens, sz.width), F32)]*2,
        compiler_params=pltpu.CompilerParams(vmem_limit_bytes=LIMIT), name="fwd")(*args)

def bwd_one(sz, scale, which, *args):
    L,D,T,F = 1, sz.width, sz.tokens, sz.hidden
    shapes = [((T,D),F32), ((L,3,D,D),BF16), ((L,D,D),BF16), ((L,D,F),BF16), ((L,D,F),BF16), ((L,6,8,D),F32), ((L,8,F),F32), ((L,3,8,D),F32), ((L,sz.groups,SLOT,WIDE),F32)]
    return pl.pallas_call(functools.partial(backward_kernel, sz, scale, which),
        out_shape=[jax.ShapeDtypeStruct(s, d) for s, d in shapes],
        in_specs=[VM]*len(args), out_specs=[VM]*len(shapes),
        scratch_shapes=[pltpu.VMEM((T,D),F32)]*2+[pltpu.VMEM((T,D),BF16), pltpu.VMEM((T,F),BF16), pltpu.VMEM((T,D),F32), pltpu.VMEM((sz.windows,SLOT,D),BF16), pltpu.VMEM((3,T,D),BF16), pltpu.VMEM((8,128),F32)],
        compiler_params=pltpu.CompilerParams(vmem_limit_bytes=LIMIT), name="bwd%d"%which)(*args)

def bwd_call(sz, scale, cot, *args):
    one = lambda which, c: bwd_one(sz, scale, which, c, *[a if a.shape[0] != 2 else a[which:which+1] for a in args])
    b = one(1, cot)
    c = one(0, b[0])
    return [c[0][:592]] + [jnp.concatenate([x, y], 0) for x, y in zip(c[1:], b[1:])]


def shards(
    block_input, cotangent, region_ids, rel_index, first_gain, first_offset, triple_weight, triple_bias, rel_table,
    project_weight, project_bias, second_gain, second_offset, expand_weight, expand_bias, reduce_weight, reduce_bias,
):
    cols = lax.axis_size("col")
    tokens = block_input.shape[0]
    mine = tokens // cols
    scale = 1.0 / math.sqrt(tokens * lax.axis_size("dp") * lax.axis_size("row"))
    sz = Sizes(mine // (SIDE * SIDE), block_input.shape[1], expand_weight.shape[2] * cols)
    held = -(-mine // 16) * 16
    start = lax.axis_index("col") * mine

    def whole(weight, last):
        return lax.all_gather(lax.all_gather(weight, "row", axis=1, tiled=True), "col", axis=last, tiled=True)

    wt = jnp.transpose(whole(triple_weight, 3), (0, 2, 1, 3))
    wp, we, wr = whole(project_weight, 2), whole(expand_weight, 2), whole(reduce_weight, 2)
    tb = lax.all_gather(triple_bias, "col", axis=2, tiled=True)
    eb = lax.all_gather(expand_bias, "col", axis=1, tiled=True)
    table = lax.all_gather(rel_table, "col", axis=2, tiled=True)
    cut = lambda rows: jnp.pad(lax.dynamic_slice_in_dim(rows, start, mine, 0), ((0, held - mine), (0, 0)))
    onehot = rel_onehot(rel_index)
    bias = jnp.stack([rel_bias(onehot, table[layer]) for layer in range(LAYERS)])
    bias = jnp.pad(bias, ((0, 0), (0, 0), (0, SLOT - CELLS), (0, 0)))
    bias = jnp.pad(bias, ((0, 0), (0, 0), (0, 0), (0, SLOT - CELLS)), constant_values=GONE)
    bias = bias.reshape(LAYERS, sz.groups, GROUP, SLOT, SLOT).transpose(0, 1, 3, 2, 4)
    bias = bias.reshape(LAYERS, sz.groups, SLOT, WIDE)
    mask = jnp.pad(region_mask(region_ids), ((0, 0), (0, SLOT - CELLS), (0, SLOT - CELLS)))
    mask = jnp.tile(mask, (1, 1, GROUP))
    heads = head_mask()
    saved = fwd_call(
        sz, cut(block_input), wt, wp, we, wr, first_gain, first_offset, tb, project_bias, second_gain, second_offset, eb,
        reduce_bias, bias, mask, heads, ones_mask(),
    )
    back = bwd_call(
        sz, scale, cut(cotangent), wt, wp, we, wr, first_gain, second_gain, heads, *saved[1:]
    )

    def rows_out(rows):
        return lax.all_gather(rows[:mine].astype(BF16), "col", axis=0, tiled=True).astype(F32)

    def scatter(grad, last):
        grad = lax.psum_scatter(grad, "row", scatter_dimension=1, tiled=True)
        grad = lax.psum_scatter(grad, "col", scatter_dimension=last, tiled=True)
        return lax.psum(grad, "dp").astype(F32)

    gt = scatter(jnp.transpose(back[1], (0, 2, 1, 3)), 3)
    gp, ge, gr = scatter(back[2], 2), scatter(back[3], 2), scatter(back[4], 2)
    small = jnp.sum(back[5], axis=2) * scale
    big = jnp.sum(back[6], axis=1) * scale
    tsum = jnp.sum(back[7], axis=2) * scale
    ssum = back[8].reshape(LAYERS, sz.groups, SLOT, GROUP, SLOT)[:, :, :CELLS, :, :CELLS]
    ssum = ssum.transpose(0, 1, 3, 2, 4).reshape(LAYERS, sz.groups * GROUP, CELLS * CELLS)
    gtab = jnp.einsum("lhp,pm->lmh", ssum, onehot, precision=lax.Precision.HIGHEST) * scale
    small, big, tsum, gtab = lax.psum((small, big, tsum, gtab), ("dp", "row", "col"))
    own = lambda value, axis: lax.dynamic_slice_in_dim(
        value, lax.axis_index("col") * (value.shape[axis] // cols), value.shape[axis] // cols, axis
    )
    return (
        rows_out(saved[0]), rows_out(back[0]), small[:, 4], small[:, 5], gt, own(tsum, 2), own(gtab, 2), gp, small[:, 3],
        small[:, 1], small[:, 2], ge, own(big, 1), gr, small[:, 0],
    )


def solution(mesh):
    specs = (
        P(("dp", "row"), None), P(("dp", "row"), None), P(), P(), P(), P(), P(None, "row", None, "col"), P(None, None, "col"),
        P(None, None, "col"), P(None, "row", "col"), P(), P(), P(), P(None, "row", "col"), P(None, "col"),
        P(None, "row", "col"), P(),
    )
    outs = specs[:2] + (
        P(), P(), P(None, "row", None, "col"), P(None, None, "col"), P(None, None, "col"), P(None, "row", "col"), P(), P(), P(),
        P(None, "row", "col"), P(None, "col"), P(None, "row", "col"), P(),
    )
    return jax.shard_map(shards, mesh=mesh, in_specs=specs, out_specs=outs, check_vma=False)
```

```python
import functools
import math
import types

import jax
import jax.numpy as jnp
from jax import lax
from jax.experimental import pallas as pl
from jax.experimental.pallas import tpu as pltpu
from jax.sharding import PartitionSpec as P

LAYERS = 2
SIDE = 14
WIN = 7
SHIFT = 3
HEAD = 32
RELS = 169
EPSILON = 1e-05
MASKED = -100.0
GONE = -1e30
CELLS = WIN * WIN
ROWS = 56
SLOT = 64
GROUP = 4
LANES = 128
WIDE = GROUP * SLOT
F32 = jnp.float32
BF16 = jnp.bfloat16
ROOT_HALF = 1.0 / math.sqrt(2.0)
GAUSS = 1.0 / math.sqrt(2.0 * math.pi)


def mm(a, b):
    return lax.dot_general(a, b, (((1,), (0,)), ((), ())), preferred_element_type=F32)


def mm_nt(a, b):
    return lax.dot_general(a, b, (((1,), (1,)), ((), ())), preferred_element_type=F32)


def mm_tn(a, b):
    return lax.dot_general(a, b, (((0,), (0,)), ((), ())), preferred_element_type=F32)


def loop(count, body):
    def step(index, carry):
        body(index)
        return carry

    lax.fori_loop(0, count, step, 0)


def span(index, size):
    return pl.ds(pl.multiple_of(index * size, size), size)


def fold(values):
    rows, columns = values.shape
    return jnp.sum(values.reshape(rows // 8, 8, columns), axis=0)


def order(images, shift):
    found = {}
    for image in range(images):
        for wi in range(2):
            for wj in range(2):
                window = image * 4 + wi * 2 + wj
                for a in range(WIN):
                    for b in range(WIN):
                        i = (wi * WIN + a + shift) % SIDE
                        j = (wj * WIN + b + shift) % SIDE
                        found[window * ROWS + a * WIN + b] = image * SIDE * SIDE + i * SIDE + j
    return found


def runs(pairs):
    joined = []
    for to, source in sorted(pairs):
        if joined and joined[-1][0] + joined[-1][2] == to and joined[-1][1] + joined[-1][2] == source:
            joined[-1][2] += 1
        else:
            joined.append([to, source, 1])
    return joined


def image_to_window(images, shift):
    return runs(order(images, shift).items())


def window_to_image(images, shift):
    return runs((source, to) for to, source in order(images, shift).items())


def window_to_window(images, before, after):
    at = {token: row for row, token in order(images, before).items()}
    return runs((row, at[token]) for row, token in order(images, after).items())


def move_rows(target, source, moves):
    for to, start, length in moves:
        target[pl.ds(to, length), :] = source[pl.ds(start, length), :]


def norm_rows(hidden, gain, offset):
    average = jnp.mean(hidden, axis=-1, keepdims=True)
    centered = hidden - average
    variance = jnp.mean(centered * centered, axis=-1, keepdims=True)
    inverse = lax.rsqrt(variance + EPSILON)
    normed = centered * inverse
    return normed * gain + offset, normed, inverse


def spread(block, mask):
    return jnp.concatenate([block] * GROUP, axis=0) * mask


def gather_heads(stacked, lane):
    out = stacked[(GROUP - 1) * SLOT :]
    for head in reversed(range(GROUP - 1)):
        out = jnp.where(lane < (head + 1) * HEAD, stacked[head * SLOT : (head + 1) * SLOT], out)
    return out


def padded(rows):
    return jnp.concatenate([rows, jnp.zeros((SLOT - ROWS, rows.shape[1]), rows.dtype)], axis=0).astype(BF16)


class Sizes:
    def __init__(self, images, width, hidden):
        self.images = images
        self.windows = images * 4
        self.tokens = self.windows * ROWS
        self.width = width
        self.hidden = hidden
        self.groups = width // LANES
        self.pairs = self.windows // 2
        self.chunk = self.tokens // 2
        self.third = self.tokens // 3


def forward_norm(sz, hidden, gain, offset, low, hat, inv):
    def body(i):
        at = span(i, 2 * ROWS)
        normed, centered, inverse = norm_rows(hidden[at, :], gain, offset)
        low[at, :] = normed.astype(BF16)
        hat[at, :] = centered.astype(BF16)
        inv[0][at, inv[1] : inv[1] + 1] = inverse

    loop(sz.pairs, body)


def forward_triple(sz, low, weight, bias, outs):
    per = sz.chunk // ROWS
    for part in range(3):

        def body(i, part=part):
            acc = mm(low[span(i, sz.chunk), :], weight[part]) + bias[part]
            if part == 0:
                acc = acc * HEAD ** (-0.5)
            for j in range(per):
                outs[part][i * per + j] = padded(acc[j * ROWS : (j + 1) * ROWS])

        loop(2, body)


def forward_attend(sz, parts, bias, mask, heads, ones, probs, out_slots, out_rows):
    query, key, value = parts

    def body(pair):
        for group in range(sz.groups):
            cols = slice(group * LANES, (group + 1) * LANES)
            halves = []
            for half in range(2):
                window = pair * 2 + half
                scores = mm_nt(query[window, :, cols], spread(key[window, :, cols], heads[...])) + bias[group]
                if mask is not None:
                    scores = scores + mask[lax.rem(window, 4)]
                grown = jnp.exp(scores)
                high = grown.astype(BF16)
                low = (grown - high.astype(F32)).astype(BF16)
                total = mm(high, ones[...]) + mm(low, ones[...])
                prob = jnp.exp(scores - jnp.log(total)).astype(BF16)
                probs[window, group] = prob
                out = mm(prob, spread(value[window, :, cols], heads[...]))
                out_slots[window, :, cols] = out.astype(BF16)
                halves.append(out[:ROWS])
            out_rows[span(pair, 2 * ROWS), cols] = jnp.concatenate(halves, axis=0).astype(BF16)

    loop(sz.pairs, body)


def add_product(sz, hidden, left, weight, bias):
    def body(i):
        at = span(i, sz.chunk)
        hidden[at, :] = hidden[at, :] + mm_nt(left[at, :], weight[...]) + bias

    loop(2, body)


def forward_expand(sz, low, weight, bias, act, slope):
    parts = sz.hidden // sz.width

    def body(i):
        rows = span(i // parts, sz.third)
        cols = span(lax.rem(i, parts), sz.width)
        u = mm(low[rows, :], weight[:, cols]) + bias(lax.rem(i, parts))
        phi = 0.5 + 0.5 * lax.erf(u * ROOT_HALF)
        act[rows, cols] = (u * phi).astype(BF16)
        slope[rows, cols] = (phi + u * (GAUSS * jnp.exp(-0.5 * u * u))).astype(BF16)

    loop(3 * parts, body)


def backward_norm(sz, upstream, grad, hat, inv, gain, sums):
    def body(i):
        at = span(i, 2 * ROWS)
        up = upstream[at, :]
        normed = hat[at, :].astype(F32)
        weighted = up * gain
        first = jnp.mean(weighted, axis=-1, keepdims=True)
        second = jnp.mean(weighted * normed, axis=-1, keepdims=True)
        grad[at, :] = grad[at, :] + inv[0][at, inv[1] : inv[1] + 1] * (weighted - first - normed * second)
        sums[0] += fold(up * normed)
        sums[1] += fold(up)

    sums[0] = jnp.zeros_like(sums[0])
    sums[1] = jnp.zeros_like(sums[1])
    loop(sz.pairs, body)


def round_grad(sz, grad, low, low_t, total):
    total[...] = jnp.zeros_like(total)

    def body(i):
        at = span(i, 2 * ROWS)
        values = grad[at, :]
        low[at, :] = values.astype(BF16)
        total[...] += fold(values)

    loop(sz.pairs, body)


def backward_hidden(sz, grad_low, weight, slope, pre_low, total):
    parts = sz.hidden // sz.width
    total[...] = jnp.zeros_like(total)

    def body(i):
        rows = span(i // parts, sz.third)
        cols = span(lax.rem(i, parts), sz.width)
        pre = mm(grad_low[rows, :], weight[:, cols]) * slope[rows, cols].astype(F32)
        pre_low[rows, cols] = pre.astype(BF16)
        total[:, cols] += fold(pre)

    loop(3 * parts, body)


def weight_grad(parts, left, right, width, out, scale):
    def body(i):
        cols = span(i, width)
        out[:, cols] = (mm_tn(left[...], right[:, cols]) * scale).astype(out.dtype)

    loop(parts, body)


def backward_out(sz, grad_low, weight, out_slots):
    per = sz.chunk // ROWS

    def body(i):
        acc = mm(grad_low[span(i, sz.chunk), :], weight[...])
        for j in range(per):
            out_slots[i * per + j] = padded(acc[j * ROWS : (j + 1) * ROWS])

    loop(2, body)


def backward_attend(sz, parts, probs, out_slots, grad_slots, heads, lane, outs, totals, score_sum):
    query, key, value = parts
    for group in range(sz.groups):
        score_sum[group] = jnp.zeros_like(score_sum[group])
    totals[...] = jnp.zeros_like(totals)

    def body(pair):
        for group in range(sz.groups):
            cols = slice(group * LANES, (group + 1) * LANES)
            halves = [[], [], []]
            for half in range(2):
                window = pair * 2 + half
                q, k, v = query[window, :, cols], key[window, :, cols], value[window, :, cols]
                prob = probs[window, group]
                grad = grad_slots[window, :, cols]
                inner = -(grad.astype(F32) * out_slots[window, :, cols].astype(F32))
                left = jnp.concatenate([grad, inner.astype(BF16)], axis=1)
                right = jnp.concatenate([spread(v, heads[...]), heads[...]], axis=1)
                score = prob.astype(F32) * mm_nt(left, right)
                score_sum[group] += score
                score_low = score.astype(BF16)
                halves[0].append((mm(score_low, spread(k, heads[...])) * HEAD ** (-0.5))[:ROWS])
                halves[1].append(gather_heads(mm_tn(score_low, q), lane)[:ROWS])
                halves[2].append(gather_heads(mm_tn(prob, grad), lane)[:ROWS])
            for part in range(3):
                joined = jnp.concatenate(halves[part], axis=0)
                at = slice(part * sz.width + group * LANES, part * sz.width + (group + 1) * LANES)
                outs[span(pair, 2 * ROWS), at] = joined.astype(BF16)
                totals[part, :, cols] += fold(joined)

    loop(sz.pairs, body)


def back_product(sz, lefts, weights, out):
    def body(i):
        at = span(i, sz.chunk)
        total = mm_nt(lefts[0][at, :], weights[0][...])
        for left, weight in zip(lefts[1:], weights[1:]):
            total = total + mm_nt(left[at, :], weight[...])
        out[at, :] = total

    loop(2, body)


def to_windows(tokens, images, offset):
    blocks = SIDE // WIN
    columns = tokens.shape[-1]
    spatial = tokens.reshape(images, SIDE, SIDE, columns)
    if offset:
        spatial = jnp.roll(spatial, (-offset, -offset), axis=(1, 2))
    spatial = spatial.reshape(images, blocks, WIN, blocks, WIN, columns).transpose(0, 1, 3, 2, 4, 5)
    return spatial.reshape(images * blocks * blocks, WIN * WIN, columns)


def region_mask(region_ids):
    cells = to_windows(region_ids.reshape(SIDE * SIDE, 1), 1, 0)[:, :, 0]
    return jnp.where(cells[:, :, None] == cells[:, None, :], 0.0, MASKED).astype(jnp.float32)


def rel_onehot(rel_index):
    return (rel_index.reshape(-1)[:, None] == jnp.arange(RELS, dtype=jnp.int32)[None, :]).astype(jnp.float32)


def rel_bias(onehot, table):
    count = table.shape[1]
    return jnp.dot(onehot, table, precision=lax.Precision.HIGHEST).T.reshape(count, WIN * WIN, WIN * WIN)


def head_mask():
    row = lax.broadcasted_iota(jnp.int32, (WIDE, LANES), 0) // SLOT
    col = lax.broadcasted_iota(jnp.int32, (WIDE, LANES), 1) // HEAD
    return jnp.where(row == col, 1.0, 0.0).astype(BF16)


def ones_mask():
    row = lax.broadcasted_iota(jnp.int32, (WIDE, WIDE), 0) // SLOT
    col = lax.broadcasted_iota(jnp.int32, (WIDE, WIDE), 1) // SLOT
    return jnp.where(row == col, 1.0, 0.0).astype(BF16)


MESH = pl.DeviceIdType.MESH
KINDS = ("r", "e", "p", "t")
LIMIT = 67_000_000
PACK = 16
SMALL = 32


class Plan:
    def __init__(self, sz, mine, ndp, nrow, ncol):
        self.sz, self.mine, self.ndp, self.nrow, self.ncol = sz, mine, ndp, nrow, ncol
        self.nj = ncol // 2
        self.held = -(-mine // 16) * 16
        self.deep = sz.width // nrow
        self.thin = sz.width // ncol
        self.broad = sz.hidden // ncol
        self.offsets = [(a, b) for a in range(nrow) for b in range(self.nj) if (a, b) != (0, 0)]
        self.nblocks = nrow * self.nj
        self.spots = self.nblocks - 1

    def block(self, kind, rows=None):
        rows = self.deep if rows is None else rows
        return {"t": (3, rows, self.thin), "p": (rows, self.thin)}.get(kind, (rows, self.broad))

    def full(self, kind):
        d, f = self.sz.width, self.sz.hidden
        return {"t": (3, d, d), "p": (d, d)}.get(kind, (d, f))

    def scratch(self):
        sz = self.sz
        T, D, F, W, G = sz.tokens, sz.width, sz.hidden, sz.windows, sz.groups
        L = LAYERS
        vm = pltpu.VMEM
        dma = lambda *shape: pltpu.SemaphoreType.DMA(shape)
        out = {}
        for kind in KINDS:
            out["w" + kind] = vm((L,) + self.full(kind), BF16)
            out["g" + kind] = vm(self.full(kind), BF16)
            out["h" + kind] = vm((L, self.nrow, self.nj) + self.block(kind), BF16)
            out["x" + kind] = vm((L, self.spots) + self.block(kind), BF16)
            out["z" + kind] = vm((L, self.ndp - 1) + self.block(kind, self.deep // self.ndp), BF16)
        out.update(
            nat_x=vm((self.held, D), BF16),
            packs=vm((self.ncol, L, PACK, 512), F32),
            table=vm((256, WIDE), F32),
            index=vm((SLOT, WIDE), jnp.int32),
            bias=vm((L, G, SLOT, WIDE), F32),
            heads=vm((WIDE, LANES), BF16),
            ones=vm((WIDE, WIDE), BF16),
            ha=vm((T, D), F32),
            hb=vm((T, D), F32),
            n1=vm((L, T, D), BF16),
            c1=vm((L, T, D), BF16),
            n2=vm((L, T, D), BF16),
            c2=vm((L, T, D), BF16),
            inv=vm((T, LANES), F32),
            q=vm((L, W, SLOT, D), BF16),
            k=vm((L, W, SLOT, D), BF16),
            v=vm((L, W, SLOT, D), BF16),
            probs=vm((L, W, G, SLOT, WIDE), BF16),
            slots=vm((L, W, SLOT, D), BF16),
            rows=vm((T, D), BF16),
            act=vm((T, F), BF16),
            slope=vm((T, F), BF16),
            low=vm((T, D), BF16),
            pre=vm((T, F), BF16),
            dslots=vm((W, SLOT, D), BF16),
            ssum=vm((L, G, SLOT, WIDE), F32),
            sums=vm((L, 6, 8, D), F32),
            wide=vm((L, 8, F), F32),
            tsum=vm((L, 3, 8, D), F32),
            sm=vm((L, SMALL, 512), F32),
            sm_pair=vm((L, SMALL, 512), F32),
            sm_plane=vm((self.nblocks, L, SMALL, 512), F32),
            sm_line=vm((self.ndp, L, SMALL, 512), F32),
            in_sem=dma(4),
            own_sem=dma(8),
            far_send=dma(8, self.spots),
            far_recv=dma(8, self.spots),
            near_send=dma(8, self.nblocks),
            near_recv=dma(8, self.nblocks),
            pack_send=dma(self.ncol),
            pack_recv=dma(self.ncol),
            half_send=dma(8, self.nblocks),
            half_recv=dma(8, self.nblocks),
            plane_send=dma(8, self.spots),
            plane_recv=dma(8, self.spots),
            line_send=dma(8, self.ndp),
            line_recv=dma(8, self.ndp),
            last_send=dma(8, self.ndp),
            last_recv=dma(8, self.ndp),
            last_own=dma(8),
            row_send=dma(2, 2 * self.nj),
            row_recv=dma(2, 2 * self.nj),
            row_own=dma(2),
            sm_send=dma(3, self.nblocks + self.ndp),
            sm_recv=dma(3, self.nblocks + self.ndp),
            spill=dma(4),
        )
        return out


def mega(plan, scale, names, *refs):
    sz = plan.sz
    inputs = ("tokens", "cot", "t_in", "p_in", "e_in", "r_in", "pack", "rel", "mask", "fg", "fo", "pb", "sg", "so", "rb")
    outputs = ("out_h", "out_g", "o_t", "o_p", "o_e", "o_r", "small", "spill_a", "spill_s")
    every = dict(zip(inputs + outputs + tuple(names), refs))
    R = types.SimpleNamespace(**every)
    for letter in "wghxz":
        setattr(R, letter, {kind: every[letter + kind] for kind in KINDS})
    R.i = {kind: every[kind + "_in"] for kind in KINDS}
    R.o = {kind: every["o_" + kind] for kind in KINDS}
    d, r, c = lax.axis_index("dp"), lax.axis_index("row"), lax.axis_index("col")
    kk, j = lax.rem(c, 2), c // 2
    T, D, F = sz.tokens, sz.width, sz.hidden
    nr, nj, ndp = plan.nrow, plan.nj, plan.ndp
    partner = (d, r, c + 1 - 2 * kk)

    def plane(offset):
        return (d, lax.rem(r + offset[0], nr), lax.rem(j + offset[1], nj) * 2 + kk)

    def source(offset):
        return lax.rem(r + nr - offset[0], nr), lax.rem(j + nj - offset[1], nj)

    def remote(src, dst, send, recv, device):
        return pltpu.make_async_remote_copy(
            src_ref=src, dst_ref=dst, send_sem=send, recv_sem=recv, device_id=device, device_id_type=MESH
        )

    def cut(ref, kind, row, col):
        rows = pl.ds(pl.multiple_of(row * plan.deep, plan.deep), plan.deep)
        width = plan.thin if kind in "tp" else plan.broad
        cols = pl.ds(pl.multiple_of(col * width, width), width)
        return ref.at[:, rows, cols] if kind == "t" else ref.at[rows, cols]

    peers = [(d, r, lax.rem(c + o, plan.ncol)) for o in range(1, plan.ncol)]
    peers += [plane(o) for o in plan.offsets if o[0]]
    peers += [(lax.rem(d + o, ndp), r, c) for o in range(1, ndp)]
    barrier = pltpu.get_barrier_semaphore()
    for peer in peers:
        pl.semaphore_signal(barrier, inc=1, device_id=peer, device_id_type=MESH)

    start = c * plan.mine
    spare = lax.rem(start, 8)
    rows_in = pl.ds(pl.multiple_of(start - spare, 8), plan.held)
    in_x = pltpu.make_async_copy(R.tokens.at[rows_in, :], R.nat_x, R.in_sem.at[0])
    in_c = pltpu.make_async_copy(R.cot.at[rows_in, :], R.low.at[0 : plan.held, :], R.in_sem.at[1])
    in_x.start()
    in_c.start()
    order_of = [(layer, kind) for layer in range(LAYERS) for kind in "tper"]
    own_copies = []
    for s, (layer, kind) in enumerate(order_of):
        copy = pltpu.make_async_copy(
            R.i[kind].at[layer], cut(R.w[kind].at[layer], kind, r, c), R.own_sem.at[s]
        )
        copy.start()
        own_copies.append(copy)
    R.packs[c] = R.pack[...]

    pl.semaphore_wait(barrier, len(peers))

    pack_copies = []
    for o in range(1, plan.ncol):
        peer = (d, r, lax.rem(c + o, plan.ncol))
        copy = remote(R.pack, R.packs.at[c], R.pack_send.at[o], R.pack_recv.at[o], peer)
        copy.start()
        pack_copies.append((o, copy))
    far_copies, near_copies = [], []
    for s, (layer, kind) in enumerate(order_of):
        own = R.i[kind].at[layer]
        here = cut(R.w[kind].at[layer], kind, r, c)
        for i, offset in enumerate(plan.offsets):
            copy = remote(own, here, R.far_send.at[s, i], R.far_recv.at[s, i], plane(offset))
            copy.start()
            far_copies.append(copy)
        copy = remote(own, here, R.near_send.at[s, plan.spots], R.near_recv.at[s, plan.spots], partner)
        copy.start()
        near_copies.append(copy)

    def weights_ready(s):
        layer, kind = order_of[s]
        whole = R.w[kind].at[layer]
        for i, offset in enumerate(plan.offsets):
            row, col = source(offset)
            here = cut(whole, kind, row, col * 2 + kk)
            remote(here, here, R.far_send.at[s, i], R.far_recv.at[s, i], partner).wait_recv()
            copy = remote(here, here, R.near_send.at[s, i], R.near_recv.at[s, i], partner)
            copy.start()
            near_copies.append(copy)
        own_copies[s].wait()
        for i, offset in enumerate(plan.offsets):
            row, col = source(offset)
            here = cut(whole, kind, row, col * 2 + 1 - kk)
            remote(here, here, R.near_send.at[s, i], R.near_recv.at[s, i], partner).wait_recv()
        here = cut(whole, kind, r, c + 1 - 2 * kk)
        remote(here, here, R.near_send.at[s, plan.spots], R.near_recv.at[s, plan.spots], partner).wait_recv()

    R.heads[...] = head_mask()
    R.ones[...] = ones_mask()
    R.index[...] = jnp.full((SLOT, WIDE), -1, jnp.int32)
    for h in range(GROUP):
        R.index[0:CELLS, h * SLOT : h * SLOT + CELLS] = R.rel[...]
    R.ha[...] = jnp.zeros((T, D), F32)
    R.hb[...] = jnp.zeros((T, D), F32)
    lane = lax.broadcasted_iota(jnp.int32, (SLOT, LANES), 1)

    def load_rows(natural, wide, target, shift):
        loop(plan.held // 16, lambda i: put(wide, i, natural))
        for gap in sorted({col * plan.mine % 8 for col in range(plan.ncol)}):

            @pl.when(spare == gap)
            def _():
                move_rows(target, wide, [(to, gap + at, n) for to, at, n in image_to_window(sz.images, shift)])

    def put(wide, i, natural):
        at = span(i, 16)
        wide[at, :] = natural[at, :].astype(F32)

    in_x.wait()
    load_rows(R.nat_x, R.hb, R.ha, 0)

    for o, _ in pack_copies:
        from_col = lax.rem(c + plan.ncol - o, plan.ncol)
        remote(R.pack, R.packs.at[from_col], R.pack_send.at[o], R.pack_recv.at[o], partner).wait_recv()
    spread_row = lax.broadcasted_iota(jnp.int32, (8, WIDE), 0)
    spread_col = lax.broadcasted_iota(jnp.int32, (8, WIDE), 1) // SLOT
    spread_heads = jnp.where(spread_row == spread_col, 1.0, 0.0).astype(BF16)
    key_lane = lax.rem(lax.broadcasted_iota(jnp.int32, (SLOT, WIDE), 1), SLOT)
    empty = jnp.where(key_lane >= CELLS, GONE, 0.0)

    def split(values):
        high = values.astype(BF16)
        rest = values - high.astype(F32)
        middle = rest.astype(BF16)
        return high, middle, (rest - middle.astype(F32)).astype(BF16)

    def make_bias(layer):
        for group in range(sz.groups):
            heads_in = R.packs[group, layer, 4:12, 0:256]
            R.table[...] = sum(mm_tn(part, spread_heads) for part in split(heads_in))

            def step(i, acc):
                for n in range(13):
                    m = i * 13 + n
                    acc = jnp.where(R.index[...] == m, R.table[pl.ds(m, 1), :], acc)
                return acc

            R.bias[layer, group] = lax.fori_loop(0, RELS // 13, step, empty)

    def lanes_of(ref_of, count):
        return jnp.concatenate([ref_of(g) for g in range(count)], axis=1)

    make_bias(0)

    for layer in range(LAYERS):
        h = R.ha if layer == 0 else R.hb
        base = 4 * layer
        row1 = slice(layer, layer + 1)
        forward_norm(sz, h, R.fg[row1, :], R.fo[row1, :], R.n1.at[layer], R.c1.at[layer], (R.inv, 2 * layer))
        weights_ready(base)
        bias3 = [lanes_of(lambda g, part=part: R.packs[g, layer, part : part + 1, 0:LANES], sz.groups) for part in range(3)]
        forward_triple(sz, R.n1.at[layer], R.w["t"].at[layer], bias3, [ref.at[layer] for ref in (R.q, R.k, R.v)])
        forward_attend(
            sz, [ref.at[layer] for ref in (R.q, R.k, R.v)], R.bias.at[layer], R.mask if layer else None, R.heads, R.ones,
            R.probs.at[layer], R.slots.at[layer], R.rows,
        )
        weights_ready(base + 1)
        add_product(sz, h, R.rows, R.w["p"].at[layer], R.pb[row1, :])
        forward_norm(sz, h, R.sg[row1, :], R.so[row1, :], R.n2.at[layer], R.c2.at[layer], (R.inv, 2 * layer + 1))
        weights_ready(base + 2)
        if layer:
            for copy in spills:
                copy.wait()
        forward_expand(sz, R.n2.at[layer], R.w["e"].at[layer], lambda n: R.packs[n, layer, 3:4, :], R.act, R.slope)
        if layer == 0:
            spills = [
                pltpu.make_async_copy(R.act, R.spill_a, R.spill.at[0]),
                pltpu.make_async_copy(R.slope, R.spill_s, R.spill.at[1]),
            ]
            for copy in spills:
                copy.start()
            make_bias(1)
        weights_ready(base + 3)
        add_product(sz, h, R.act, R.w["r"].at[layer], R.rb[row1, :])
        if layer == 0:
            R.hb[...] = jnp.zeros((T, D), F32)
            move_rows(R.hb, R.ha, window_to_window(sz.images, 0, SHIFT))

    def send_rows(which, natural, wide, out):
        def narrow(i):
            at = span(i, 16)
            natural[at, :] = wide[at, :].astype(BF16)

        loop(plan.held // 16, narrow)
        own = pltpu.make_async_copy(natural, out.at[c], R.row_own.at[which])
        own.start()
        copies = []
        for b in range(1, nj):
            copies.append(remote(natural, out.at[c], R.row_send.at[which, b], R.row_recv.at[which, b], plane((0, b))))
        copies.append(remote(natural, out.at[c], R.row_send.at[which, 0], R.row_recv.at[which, 0], partner))
        for copy in copies:
            copy.start()
        return own, copies

    def relay_rows(which, natural, out):
        copies = []
        for b in range(1, nj):
            at = out.at[lax.rem(j + nj - b, nj) * 2 + kk]
            remote(natural, at, R.row_send.at[which, b], R.row_recv.at[which, b], partner).wait_recv()
            copy = remote(at, at, R.row_send.at[which, nj + b], R.row_recv.at[which, nj + b], partner)
            copy.start()
            copies.append(copy)
        return copies

    def finish_rows(which, natural, out, own, copies):
        own.wait()
        for copy in copies:
            copy.wait_send()
        at = out.at[c + 1 - 2 * kk]
        remote(natural, at, R.row_send.at[which, 0], R.row_recv.at[which, 0], partner).wait_recv()
        for b in range(1, nj):
            at = out.at[lax.rem(j + nj - b, nj) * 2 + 1 - kk]
            remote(natural, at, R.row_send.at[which, nj + b], R.row_recv.at[which, nj + b], partner).wait_recv()

    move_rows(R.ha, R.hb, window_to_image(sz.images, SHIFT))
    own_h, sent_h = send_rows(0, R.nat_x, R.ha, R.out_h)
    for copy in far_copies + near_copies:
        copy.wait_send()
    for _, copy in pack_copies:
        copy.wait_send()

    pending = []

    def stage_half(kind, layer):
        n = KINDS.index(kind) * 2 + layer
        for a in range(nr):
            for b in range(nj):
                i = a * nj + b
                copy = remote(
                    cut(R.g[kind], kind, a, 2 * b + 1 - kk), R.h[kind].at[layer, a, b],
                    R.half_send.at[n, i], R.half_recv.at[n, i], partner,
                )
                copy.start()

    def stage_plane(kind, layer):
        n = KINDS.index(kind) * 2 + layer
        for a in range(nr):
            for b in range(nj):
                i = a * nj + b
                copy = remote(
                    cut(R.g[kind], kind, a, 2 * b + 1 - kk), R.h[kind].at[layer, a, b],
                    R.half_send.at[n, i], R.half_recv.at[n, i], partner,
                )
                copy.wait()
                add_blocks(plan, kind, R.h[kind].at[layer, a, b], [cut(R.g[kind], kind, a, 2 * b + kk)])
        for i, offset in enumerate(plan.offsets):
            row, col = lax.rem(r + offset[0], nr), lax.rem(j + offset[1], nj)
            copy = remote(
                R.h[kind].at[layer, row, col], R.x[kind].at[layer, i],
                R.plane_send.at[n, i], R.plane_recv.at[n, i], plane(offset),
            )
            copy.start()
            pending.append(copy)

    step_rows = plan.deep // ndp

    def part(ref, kind, index):
        rows = pl.ds(pl.multiple_of(index * step_rows, step_rows), step_rows)
        return ref.at[:, rows, :] if kind == "t" else ref.at[rows, :]

    def stage_line(kind, layer):
        n = KINDS.index(kind) * 2 + layer
        own = R.h[kind].at[layer, r, j]
        for i, offset in enumerate(plan.offsets):
            there = R.x[kind].at[layer, i]
            remote(there, there, R.plane_send.at[n, i], R.plane_recv.at[n, i], partner).wait_recv()
        add_blocks(plan, kind, own, [R.x[kind].at[layer, i] for i in range(plan.spots)])
        for o in range(1, ndp):
            to = lax.rem(d + o, ndp)
            copy = remote(
                part(own, kind, to), R.z[kind].at[layer, o - 1], R.line_send.at[n, o], R.line_recv.at[n, o], (to, r, c)
            )
            copy.start()
            pending.append(copy)

    def stage_last(kind, layer):
        n = KINDS.index(kind) * 2 + layer
        own = part(R.h[kind].at[layer, r, j], kind, d)
        for o in range(1, ndp):
            there = R.z[kind].at[layer, o - 1]
            remote(there, there, R.line_send.at[n, o], R.line_recv.at[n, o], partner).wait_recv()
        add_blocks(plan, kind, own, [R.z[kind].at[layer, i] for i in range(ndp - 1)])
        there = part(R.o[kind].at[layer], kind, d)
        copy = pltpu.make_async_copy(own, there, R.last_own.at[n])
        copy.start()
        for o in range(1, ndp):
            to = (lax.rem(d + o, ndp), r, c)
            copy = remote(own, there, R.last_send.at[n, o], R.last_recv.at[n, o], to)
            copy.start()
            pending.append(copy)

    def stage_end(kind, layer):
        n = KINDS.index(kind) * 2 + layer
        own = part(R.h[kind].at[layer, r, j], kind, d)
        pltpu.make_async_copy(own, part(R.o[kind].at[layer], kind, d), R.last_own.at[n]).wait()
        for o in range(1, ndp):
            there = part(R.o[kind].at[layer], kind, lax.rem(d + ndp - o, ndp))
            remote(own, there, R.last_send.at[n, o], R.last_recv.at[n, o], partner).wait_recv()

    in_c.wait()
    R.hb[...] = jnp.zeros((T, D), F32)
    load_rows(R.low, R.ha, R.hb, SHIFT)
    for layer in reversed(range(LAYERS)):
        e, dn = (R.hb, R.ha) if layer else (R.ha, R.hb)
        row1 = slice(layer, layer + 1)
        inv1 = (R.inv, 2 * layer)
        inv2 = (R.inv, 2 * layer + 1)
        sums = R.sums.at[layer]
        first = layer == LAYERS - 1
        round_grad(sz, e, R.low, None, sums.at[0])
        if not first:
            for copy in fills:
                copy.wait()
        weight_grad(F // D, R.low, R.act, D, R.g["r"], scale)
        stage_half("r", layer)
        backward_hidden(sz, R.low, R.w["r"].at[layer], R.slope, R.pre, R.wide.at[layer])
        if first:
            fills = [
                pltpu.make_async_copy(R.spill_a, R.act, R.spill.at[2]),
                pltpu.make_async_copy(R.spill_s, R.slope, R.spill.at[3]),
            ]
            for copy in fills:
                copy.start()
            relayed_h = relay_rows(0, R.nat_x, R.out_h)
        else:
            stage_line("t", 1)
        weight_grad(F // D, R.n2.at[layer], R.pre, D, R.g["e"], scale)
        stage_half("e", layer)
        stage_plane("r", layer)
        back_product(sz, [R.pre], [R.w["e"].at[layer]], dn)
        backward_norm(sz, dn, e, R.c2.at[layer], inv2, R.sg[row1, :], sums.at[1:3])
        round_grad(sz, e, R.low, None, sums.at[3])
        collect_rows(sz, R.slots.at[layer], R.rows)
        weight_grad(1, R.low, R.rows, D, R.g["p"], scale)
        stage_half("p", layer)
        stage_plane("e", layer)
        if not first:
            stage_last("t", 1)
        backward_out(sz, R.low, R.w["p"].at[layer], R.dslots)
        stage_line("r", layer)
        stage_plane("p", layer)
        backward_attend(
            sz, [ref.at[layer] for ref in (R.q, R.k, R.v)], R.probs.at[layer], R.slots.at[layer], R.dslots, R.heads, lane,
            R.pre, R.tsum.at[layer], R.ssum.at[layer],
        )
        stage_line("e", layer)
        stage_last("r", layer)
        for piece in range(3):
            cols = slice(piece * D, (piece + 1) * D)
            weight_grad(1, R.n1.at[layer], R.pre.at[:, cols], D, R.g["t"].at[piece], scale)
        stage_half("t", layer)
        stage_line("p", layer)
        back_product(
            sz, [R.pre.at[:, p * D : (p + 1) * D] for p in range(3)], [R.w["t"].at[layer, p] for p in range(3)], dn
        )
        stage_plane("t", layer)
        backward_norm(sz, dn, e, R.c1.at[layer], inv1, R.fg[row1, :], sums.at[4:6])
        stage_last("e", layer)
        stage_last("p", layer)
        if layer:
            R.ha[...] = jnp.zeros((T, D), F32)
            move_rows(R.ha, R.hb, window_to_window(sz.images, SHIFT, 0))
    move_rows(R.hb, R.ha, window_to_image(sz.images, 0))
    finish_rows(0, R.nat_x, R.out_h, own_h, sent_h + relayed_h)
    own_g, sent_g = send_rows(1, R.nat_x, R.hb, R.out_g)

    R.sm[...] = jnp.zeros(R.sm.shape, F32)
    for layer in range(LAYERS):
        sm = R.sm.at[layer]
        for row, at in enumerate((4, 5, None, None, None, 3, 1, 2, 0)):
            if at is not None:
                sm[row : row + 1, :] = jnp.sum(R.sums[layer, at], axis=0, keepdims=True) * scale
        for p in range(3):
            sm[2 + p : 3 + p, :] = jnp.sum(R.tsum[layer, p], axis=0, keepdims=True) * scale
        for p in range(F // D):
            cols = slice(p * D, (p + 1) * D)
            sm[9 + p : 10 + p, :] = jnp.sum(R.wide[layer, :, cols], axis=0, keepdims=True) * scale

    def table_grads(layer):
        for group in range(sz.groups):
            R.table[...] = jnp.zeros((256, WIDE), F32)

            def step(i):
                for n in range(13):
                    m = i * 13 + n
                    chosen = jnp.where(R.index[...] == m, R.ssum[layer, group], 0.0)
                    R.table[pl.ds(m, 1), :] = jnp.sum(chosen, axis=0, keepdims=True)

            loop(RELS // 13, step)
            total = sum(mm_nt(spread_heads, p) for p in split(R.table[...]))
            at = 16 + GROUP * group
            R.sm[layer, at : at + GROUP, 0:256] = total[0:GROUP] * scale

    table_grads(1)
    stage_line("t", 0)
    relayed_g = relay_rows(1, R.nat_x, R.out_g)
    table_grads(0)
    pair = remote(R.sm, R.sm_pair, R.sm_send.at[0, 0], R.sm_recv.at[0, 0], partner)
    pair.start()
    stage_last("t", 0)
    pair.wait()
    own = R.sm_plane.at[r * nj + j]
    own[...] = R.sm[...] + R.sm_pair[...]
    for i, offset in enumerate(plan.offsets):
        copy = remote(own, own, R.sm_send.at[1, i], R.sm_recv.at[1, i], plane(offset))
        copy.start()
        pending.append(copy)
    for i, offset in enumerate(plan.offsets):
        row, col = source(offset)
        there = R.sm_plane.at[row * nj + col]
        remote(there, there, R.sm_send.at[1, i], R.sm_recv.at[1, i], partner).wait_recv()
    own = R.sm_line.at[d]
    own[...] = sum(R.sm_plane[i] for i in range(plan.nblocks))
    for o in range(1, ndp):
        to = (lax.rem(d + o, ndp), r, c)
        copy = remote(own, own, R.sm_send.at[2, o], R.sm_recv.at[2, o], to)
        copy.start()
        pending.append(copy)
    for o in range(1, ndp):
        there = R.sm_line.at[lax.rem(d + ndp - o, ndp)]
        remote(there, there, R.sm_send.at[2, o], R.sm_recv.at[2, o], partner).wait_recv()
    R.small[...] = sum(R.sm_line[i] for i in range(ndp))
    finish_rows(1, R.nat_x, R.out_g, own_g, sent_g + relayed_g)
    for kind in KINDS:
        for layer in range(LAYERS):
            stage_end(kind, layer)
    for copy in pending:
        copy.wait_send()


def add_blocks(plan, kind, into, others):
    rows = into.shape[-2]
    step = min(64, rows)
    planes = range(into.shape[0]) if kind == "t" else (None,)
    for p in planes:

        def body(i, p=p):
            at = (span(i, step), slice(None)) if p is None else (p, span(i, step), slice(None))
            total = into[at].astype(F32)
            for other in others:
                total = total + other[at].astype(F32)
            into[at] = total.astype(BF16)

        loop(rows // step, body)


def collect_rows(sz, slots, rows):
    def body(pair):
        halves = [slots[pair * 2 + half].astype(F32)[:ROWS] for half in range(2)]
        rows[span(pair, 2 * ROWS), :] = jnp.concatenate(halves, axis=0).astype(BF16)

    loop(sz.pairs, body)


def shards(
    block_input, cotangent, region_ids, rel_index, first_gain, first_offset, triple_weight, triple_bias, rel_table,
    project_weight, project_bias, second_gain, second_offset, expand_weight, expand_bias, reduce_weight, reduce_bias,
):
    ndp, nrow, ncol = (lax.axis_size(name) for name in ("dp", "row", "col"))
    tokens = block_input.shape[0]
    mine = tokens // ncol
    scale = 1.0 / math.sqrt(tokens * ndp * nrow)
    sz = Sizes(mine // (SIDE * SIDE), block_input.shape[1], expand_weight.shape[2] * ncol)
    plan = Plan(sz, mine, ndp, nrow, ncol)
    pad = lambda value: jnp.pad(value, ((0, 0), (0, 0), (0, 512 - value.shape[2])))
    pack = jnp.concatenate(
        [pad(triple_bias), pad(expand_bias[:, None]), pad(jnp.transpose(rel_table, (0, 2, 1))), jnp.zeros((LAYERS, 8, 512), F32)], axis=1
    )
    mask = jnp.pad(region_mask(region_ids), ((0, 0), (0, SLOT - CELLS), (0, SLOT - CELLS)))
    mask = jnp.tile(mask, (1, 1, GROUP))
    vmem = pl.BlockSpec(memory_space=pltpu.VMEM)
    hbm = pl.BlockSpec(memory_space=pl.ANY)
    scratch = plan.scratch()
    D, T, F = sz.width, sz.tokens, sz.hidden
    outs = [((ncol, plan.held, D), BF16)] * 2
    outs += [((LAYERS,) + plan.block(kind), BF16) for kind in "tper"]
    outs += [((LAYERS, SMALL, 512), F32), ((T, F), BF16), ((T, F), BF16)]
    got = pl.pallas_call(
        functools.partial(mega, plan, scale, tuple(scratch)),
        out_shape=[jax.ShapeDtypeStruct(*o) for o in outs],
        in_specs=[hbm] * 6 + [vmem] * 9,
        out_specs=[hbm] * 6 + [vmem] + [hbm] * 2,
        scratch_shapes=list(scratch.values()),
        compiler_params=pltpu.CompilerParams(collective_id=0, has_side_effects=True, vmem_limit_bytes=LIMIT),
        name="blocks",
    )(
        block_input, cotangent, jnp.transpose(triple_weight, (0, 2, 1, 3)), project_weight, expand_weight, reduce_weight, pack,
        rel_index, mask, first_gain, first_offset, project_bias, second_gain, second_offset, reduce_bias,
    )
    out_h, out_g, gt, gp, ge, gr, small = got[:7]
    whole = lambda rows: rows[:, :mine].reshape(tokens, D).astype(F32)
    col = lax.axis_index("col")
    tri = lax.dynamic_slice_in_dim(small[:, 2:5], col * plan.thin, plan.thin, 2)
    wide = lax.dynamic_slice_in_dim(small, 9 + col, 1, 1)[:, 0]
    heads = lax.dynamic_slice_in_dim(small[:, 16:32, :RELS], col * (16 // ncol), 16 // ncol, 1)
    return (
        whole(out_h), whole(out_g), small[:, 0], small[:, 1], jnp.transpose(gt, (0, 2, 1, 3)).astype(F32), tri,
        jnp.transpose(heads, (0, 2, 1)), gp.astype(F32), small[:, 5], small[:, 6], small[:, 7], ge.astype(F32), wide,
        gr.astype(F32), small[:, 8],
    )


def solution(mesh):
    specs = (
        P(("dp", "row"), None), P(("dp", "row"), None), P(), P(), P(), P(), P(None, "row", None, "col"), P(None, None, "col"),
        P(None, None, "col"), P(None, "row", "col"), P(), P(), P(), P(None, "row", "col"), P(None, "col"),
        P(None, "row", "col"), P(),
    )
    outs = specs[:2] + (
        P(), P(), P(None, "row", None, "col"), P(None, None, "col"), P(None, None, "col"), P(None, "row", "col"), P(), P(), P(),
        P(None, "row", "col"), P(None, "col"), P(None, "row", "col"), P(),
    )
    return jax.shard_map(shards, mesh=mesh, in_specs=specs, out_specs=outs, check_vma=False)
```
